32 devices in a mesh: groups: 2 (over y), row: 8 (over z, x), head: 2 (over core).
Axes of the slice: x: 2, y: 2, z: 4, core: 2. Of those that a mesh axis runs over, the one named last changes fastest.
Arguments:
- pair: bfloat16 [64, 32, 128], P(('groups', 'row')), parts along dimension 0
- mask: int32 [64], P('groups'), parts along dimension 0, may hold values from 0 to 1, as said below
- ln_gain: float32 [128], replicated, may hold values from 0.5 to 1.5
- ln_bias: float32 [128], replicated, may hold values from -3 to 3
- w_query: bfloat16 [128, 128], P(None, 'head'), may hold values from -0.5 to 0.5
- w_key: bfloat16 [128, 128], P(None, 'head'), may hold values from -0.5 to 0.5
- w_value: bfloat16 [128, 128], P(None, 'head'), may hold values from -0.5 to 0.5
- w_bias: bfloat16 [128, 4], P(None, 'head')
- w_gate: bfloat16 [128, 128], P(None, 'head'), may hold values from -0.5 to 0.5
- gate_bias: float32 [128], P('head'), may hold values from -4 to 4
- w_out: bfloat16 [128, 128], P('head'), may hold values from -0.5 to 0.5
- out_bias: float32 [128], replicated, may hold values from -3 to 3
Outputs:
- result: bfloat16 [64, 32, 128], P(('groups', 'row'), 'head'), parts along dimension 0
The draws below stay inside these ranges and needn't reach their ends.
There are 2 independent parts, one for each index of `groups`. The reference program is written for one: setup_inputs(seed, part) draws one part's arguments, and reference() takes and returns one part's arrays. A program takes and returns all parts, laid end to end along the dimension named above; an argument that names none is the same for every part. Nothing has to cross between parts.
Inputs may be any that keep to these rules, and one draw needn't show every extreme that they name: mask is 1 on a leading run of at least 16 entries and 0 after it.
All inputs are finite; a program needn't handle non-finite values.
Results may differ from the reference program's by a relative error of at most 0.012.
The reference program's roundings to bfloat16 on the way (of `normed`, `query`, `weights` and `gated`) count: a program that leaves them out, or rounds other values in their place, can miss the bound.
Values may be sent and summed in bfloat16 or wider, within the bound.
A program may use at most 64 MiB of HBM per device.

```python
import math
import jax
import jax.numpy as jnp
from jax import lax

C = 128
HEADS = 4
HD = 32
N = 32


def draw_pair(key, part):
    base = jax.random.normal(key, (N, N, C), jnp.float32)
    return base.astype(jnp.bfloat16)


def draw_mask(key, part):
    length = jax.random.randint(jax.random.fold_in(key, 11), (), N // 2, N + 1)
    return (jnp.arange(N) < length).astype(jnp.int32)


def draw_w_bias(key, part):
    weights = jax.random.normal(jax.random.fold_in(key, 13), (C, HEADS), jnp.float32) / math.sqrt(C)
    return weights.astype(jnp.bfloat16)


def steps_of(rng, shape, cuts, smallest, largest):
    def one(dim, parts):
        steps = jax.random.uniform(jax.random.fold_in(jax.random.fold_in(rng, 6), dim), (parts,), jnp.float32, smallest / len(cuts), largest / len(cuts))
        return jnp.repeat(jnp.exp(steps), shape[dim] // parts).reshape((-1,) + (1,) * (len(shape) - dim - 1))

    level = one(*cuts[0])
    for cut in cuts[1:]:
        level = level * one(*cut)
    return level


def noise(rng, dims, scale, most, cuts=(), kind=jnp.bfloat16):
    entries = scale * jax.random.normal(rng, dims, jnp.float32)
    if cuts:
        entries = entries * steps_of(rng, dims, cuts, -0.22, 0.18)
    return jnp.clip(entries, -most, most).astype(kind)


def setup_inputs(seed: int = 0, part: int = 0) -> dict:
    streams_of = jax.random.split(jax.random.key(seed), 13)
    part_keys = jax.random.split(jax.random.fold_in(streams_of[12], part), 13)
    pair = draw_pair(jax.random.fold_in(jax.random.fold_in(streams_of[12], part), 71), part)
    mask = draw_mask(jax.random.fold_in(jax.random.fold_in(streams_of[12], part), 71), part)
    ln_gain = jnp.clip(1.0 + 0.1 * jax.random.normal(streams_of[2], (C,), jnp.float32), 0.5, 1.5)
    ln_bias = noise(streams_of[3], (C,), 0.5, 3.0, (), jnp.float32)
    w_query = noise(streams_of[4], (C, HEADS * HD), C ** -0.5, 0.5, ((1, 2),))
    w_key = noise(streams_of[5], (C, HEADS * HD), C ** -0.5, 0.5, ((1, 2),))
    w_value = noise(streams_of[6], (C, HEADS * HD), C ** -0.5, 0.5, ((1, 2),))
    w_bias = draw_w_bias(jax.random.fold_in(streams_of[12], 71), part)
    w_gate = noise(streams_of[8], (C, HEADS * HD), C ** -0.5, 0.5, ((1, 2),))
    gate_bias = noise(streams_of[9], (HEADS * HD,), 1.0, 4.0, ((0, 2),), jnp.float32)
    w_out = noise(streams_of[10], (HEADS * HD, C), (HEADS * HD) ** -0.5, 0.5, ((0, 2),))
    out_bias = noise(streams_of[11], (C,), 0.5, 3.0, (), jnp.float32)
    return {"pair": pair, "mask": mask, "ln_gain": ln_gain, "ln_bias": ln_bias, "w_query": w_query, "w_key": w_key, "w_value": w_value, "w_bias": w_bias, "w_gate": w_gate, "gate_bias": gate_bias, "w_out": w_out, "out_bias": out_bias}


EPSILON = 1e-05
MASK_WEIGHT = 1000000000.0

def layer_normed(pair_rows, ln_gain, ln_bias):
    values_f = pair_rows.astype(jnp.float32)
    average = lax.optimization_barrier(jnp.mean(values_f, axis=-1, keepdims=True))
    centred = values_f - average
    variance = lax.optimization_barrier(jnp.mean(centred * centred, axis=-1, keepdims=True))
    scaled = centred * lax.rsqrt(variance + EPSILON) * ln_gain.astype(jnp.float32) + ln_bias.astype(jnp.float32)
    return scaled.astype(jnp.bfloat16)

def reference(pair, mask, ln_gain, ln_bias, w_query, w_key, w_value, w_bias, w_gate, gate_bias, w_out, out_bias):
    normed = lax.map(lambda pair_row: layer_normed(pair_row, ln_gain, ln_bias), pair)
    bias = lax.map(lambda pair_row: jnp.dot(pair_row, w_bias, preferred_element_type=jnp.float32), normed)
    bias = jnp.transpose(bias, (2, 0, 1))
    mask_add = (mask.astype(jnp.float32) - 1.0) * MASK_WEIGHT
    scale = HD ** (-0.5)
    width_all = pair.shape[1]

    def one_row(pair_row):
        query = (jnp.dot(pair_row, w_query, preferred_element_type=jnp.float32) * scale).astype(jnp.bfloat16)
        query = query.reshape(width_all, HEADS, HD)
        keys_all = jnp.dot(pair_row, w_key, preferred_element_type=jnp.float32).astype(jnp.bfloat16)
        keys_all = keys_all.reshape(width_all, HEADS, HD)
        values_all = jnp.dot(pair_row, w_value, preferred_element_type=jnp.float32).astype(jnp.bfloat16)
        values_all = values_all.reshape(width_all, HEADS, HD)
        gate = jax.nn.sigmoid(jnp.dot(pair_row, w_gate, preferred_element_type=jnp.float32) + gate_bias.astype(jnp.float32))
        scores = jnp.einsum('jhd,khd->hjk', query.astype(jnp.float32), keys_all.astype(jnp.float32))
        scores = scores + bias + mask_add
        highest = lax.optimization_barrier(jnp.max(scores, axis=-1, keepdims=True))
        exponent = jnp.exp(scores - highest)
        weights = (exponent / lax.optimization_barrier(jnp.sum(exponent, axis=-1, keepdims=True))).astype(jnp.bfloat16)
        attended = jnp.einsum('hjk,khd->jhd', weights.astype(jnp.float32), values_all.astype(jnp.float32))
        gated = (gate * attended.reshape(width_all, HEADS * HD)).astype(jnp.bfloat16)
        mixed = jnp.dot(gated, w_out, preferred_element_type=jnp.float32) + out_bias.astype(jnp.float32)
        return mixed.astype(jnp.bfloat16)
    return lax.map(one_row, normed)
```

```python
import functools
import math

import jax
import jax.numpy as jnp
from jax import lax
from jax.experimental import pallas as pl
from jax.experimental.pallas import tpu as pltpu
from jax.sharding import PartitionSpec as P

HD = 32


EPSILON = 1e-05
MASK_WEIGHT = 1000000000.0


def layer_normed(pair_rows, ln_gain, ln_bias):
    values_f = pair_rows.astype(jnp.float32)
    average = jnp.mean(values_f, axis=-1, keepdims=True)
    centred = values_f - average
    variance = jnp.mean(centred * centred, axis=-1, keepdims=True)
    scaled = centred * lax.rsqrt(variance + EPSILON) * ln_gain + ln_bias
    return scaled.astype(jnp.bfloat16)


def attend_rows(result, bias_block, offset, query, keys_all, values_all, mask_add):
    sub_rows = bias_block.shape[1]
    query_block = lax.dynamic_slice_in_dim(query, offset, sub_rows, 1)
    scores = jnp.einsum(
        "ijhd,ikhd->ihjk", query_block, keys_all, preferred_element_type=jnp.float32
    )
    scores = scores + bias_block[None] + mask_add
    highest = jnp.max(scores, axis=-1, keepdims=True)
    exponent = jnp.exp(scores - highest)
    weights = (exponent / jnp.sum(exponent, axis=-1, keepdims=True)).astype(jnp.bfloat16)
    attended = jnp.einsum(
        "ihjk,ikhd->ijhd", weights, values_all, preferred_element_type=jnp.float32
    )
    return lax.dynamic_update_slice_in_dim(result, attended, offset, 1)


def attend_block(carry, piece, start, block_rows, query, keys_all, values_all, mask_add):
    count = piece.shape[1]

    def one_step(turn, result):
        offset = turn * block_rows
        bias_block = lax.dynamic_slice_in_dim(piece, offset, block_rows, 1)
        return attend_rows(
            result, bias_block, start + offset, query, keys_all, values_all, mask_add
        )

    return lax.fori_loop(0, count // block_rows, one_step, carry)


def local(
    pair,
    mask,
    ln_gain,
    ln_bias,
    w_query,
    w_key,
    w_value,
    w_bias,
    w_gate,
    gate_bias,
    w_out,
    out_bias,
):
    local_rows, width_all, channels = pair.shape
    normed = layer_normed(pair, ln_gain, ln_bias)
    flat = normed.reshape(-1, channels)
    inner_width = w_query.shape[1]
    heads_local = inner_width // HD
    joined = jnp.concatenate([w_query, w_key, w_value, w_gate], axis=1)
    projected = jnp.dot(flat, joined, preferred_element_type=jnp.float32)
    four_shape = (local_rows, width_all, heads_local, HD)
    query = (projected[:, :inner_width] * HD ** (-0.5)).astype(jnp.bfloat16).reshape(four_shape)
    keys_all = projected[:, inner_width : 2 * inner_width].astype(jnp.bfloat16).reshape(four_shape)
    values_all = (
        projected[:, 2 * inner_width : 3 * inner_width].astype(jnp.bfloat16).reshape(four_shape)
    )
    gate = jax.nn.sigmoid(projected[:, 3 * inner_width :] + gate_bias)
    bias_local = jnp.dot(flat, w_bias, preferred_element_type=jnp.float32)
    bias_local = jnp.transpose(bias_local.reshape(local_rows, width_all, heads_local), (2, 0, 1))
    mask_add = (mask.astype(jnp.float32) - 1.0) * MASK_WEIGHT
    block_rows = math.gcd(width_all, 64)
    empty = jnp.zeros(four_shape, jnp.float32)
    bias_every = lax.all_gather(bias_local, "row", axis=1, tiled=True)
    attended = attend_block(empty, bias_every, 0, block_rows, query, keys_all, values_all, mask_add)
    gated = (gate * attended.reshape(-1, inner_width)).astype(jnp.bfloat16)
    traded = lax.all_to_all(
        gated.reshape(local_rows, width_all, inner_width),
        "head",
        split_axis=1,
        concat_axis=2,
        tiled=True,
    )
    out_full = lax.all_gather(w_out, "head", axis=0, tiled=True)
    mixed = jnp.dot(
        traded.reshape(-1, traded.shape[2]), out_full, preferred_element_type=jnp.float32
    )
    mixed = mixed.reshape(local_rows, traded.shape[1], channels)
    return (mixed + out_bias).astype(jnp.bfloat16)


LANES = 128
SUBLANES = 8
MESH = pl.DeviceIdType.MESH


def packs(mesh, pair, w_query):
    rows, heads = mesh.shape["row"], mesh.shape["head"]
    part_rows = pair.shape[0] // mesh.shape["groups"]
    width, channels = pair.shape[1:]
    local_rows = part_rows // rows
    return (
        heads == 2
        and part_rows == width
        and rows % heads == 0
        and SUBLANES % local_rows == 0
        and width % (16 * heads) == 0
        and channels == LANES
        and w_query.shape[1] == LANES
        and (LANES // HD) * width == LANES
    )


def packed_kernel(
    n_row,
    pair_h,
    mask_h,
    gain_h,
    shift_h,
    wq_h,
    wk_h,
    wv_h,
    wb_h,
    wg_h,
    gb_h,
    wo_h,
    ob_h,
    out_ref,
    pair_v,
    mask_v,
    gain_v,
    shift_v,
    wq_v,
    wk_v,
    wv_v,
    wb_v,
    wg_v,
    gb_v,
    wo_v,
    ob_v,
    normed_v,
    message,
    received,
    in_sem,
    w_send,
    w_recv,
    b_send,
    b_recv,
):
    row, core = lax.axis_index("row"), lax.axis_index("head")
    other = 1 - core
    local_rows, width, channels = pair_v.shape
    inner = wq_v.shape[2]
    part = width // 2
    per_half = n_row // 2
    half = row // per_half
    heads_local = wb_v.shape[1]
    f32, bf16 = jnp.float32, jnp.bfloat16

    barrier = pltpu.get_barrier_semaphore()
    for slot in range(n_row):
        src_row, src_core = core * per_half + slot // 2, slot % 2

        @pl.when(jnp.logical_or(src_row != row, src_core != core))
        def _():
            pl.semaphore_signal(
                barrier,
                inc=1,
                device_id={"row": src_row, "head": src_core},
                device_id_type=MESH,
            )

    @pl.when(half != core)
    def _():
        pl.semaphore_signal(
            barrier, inc=1, device_id={"row": row, "head": other}, device_id_type=MESH
        )

    locals_ = [
        pltpu.make_async_copy(src, dst, in_sem.at[i])
        for i, (src, dst) in enumerate(
            (
                (pair_h, pair_v),
                (gain_h, gain_v),
                (shift_h, shift_v),
                (wb_h, wb_v),
                (mask_h, mask_v),
                (ob_h, ob_v),
                (wk_h, wk_v.at[core]),
                (wq_h, wq_v.at[core]),
                (wv_h, wv_v.at[core]),
                (wg_h, wg_v.at[core]),
                (gb_h, gb_v.at[core]),
                (wo_h, wo_v.at[core]),
            )
        )
    ]
    for copy in locals_:
        copy.start()
    weights = [
        pltpu.make_async_remote_copy(
            src_ref=src,
            dst_ref=dst.at[core],
            send_sem=w_send.at[i],
            recv_sem=w_recv.at[i],
            device_id={"row": row, "head": other},
            device_id_type=MESH,
        )
        for i, (src, dst) in enumerate(
            (
                (wk_h, wk_v),
                (wq_h, wq_v),
                (wv_h, wv_v),
                (wg_h, wg_v),
                (gb_h, gb_v),
                (wo_h, wo_v),
            )
        )
    ]

    for copy in locals_[:4]:
        copy.wait()
    lane_head = lax.broadcasted_iota(jnp.int32, (channels, LANES), 1) // width
    wb = wb_v[...]
    spread = jnp.zeros((channels, LANES), f32)
    for h in range(heads_local):
        column = jnp.broadcast_to(wb[:, h : h + 1].astype(f32), (channels, LANES))
        spread = jnp.where(lane_head == core * heads_local + h, column, spread)
    spread = spread.astype(bf16)
    values_f = pair_v[...].astype(f32).reshape(local_rows * width, channels)
    average = jnp.mean(values_f, axis=-1, keepdims=True)
    centred = values_f - average
    variance = jnp.mean(centred * centred, axis=-1, keepdims=True)
    normed = (centred * lax.rsqrt(variance + EPSILON) * gain_v[...] + shift_v[...]).astype(bf16)
    normed_v[...] = normed.reshape(local_rows, width, channels)

    product = jnp.dot(normed, spread, preferred_element_type=f32)
    tokens = local_rows * width
    token_key = lax.broadcasted_iota(jnp.int32, (tokens, LANES), 0) % width
    lane_key = lax.broadcasted_iota(jnp.int32, (tokens, LANES), 1) % width
    product = jnp.where(token_key == lane_key, product, 0.0)
    reduced = jnp.sum(product.reshape(local_rows, width, LANES), axis=1)
    per_tile = SUBLANES // local_rows
    sublane = lax.broadcasted_iota(jnp.int32, (SUBLANES, LANES), 0)
    tile = jnp.zeros((SUBLANES, LANES), f32)
    for j in range(local_rows):
        tile = jnp.where(sublane == (row % per_tile) * local_rows + j, reduced[j : j + 1], tile)
    message[...] = tile

    pl.semaphore_wait(barrier, n_row)
    slot_mine = (row % per_half) * 2 + core

    def bias_copy(turn):
        return pltpu.make_async_remote_copy(
            src_ref=message,
            dst_ref=received.at[slot_mine],
            send_sem=b_send.at[turn],
            recv_sem=b_recv.at[slot_mine],
            device_id={"row": lax.rem(row + turn, n_row), "head": half},
            device_id_type=MESH,
        )

    for turn in reversed(range(1, n_row)):
        bias_copy(turn).start()

    @pl.when(half != core)
    def _():
        bias_copy(0).start()

    for copy in weights:
        copy.start()

    @pl.when(half == core)
    def _():
        received[slot_mine] = tile

    for copy in locals_[4:]:
        copy.wait()
    for copy in weights:
        copy.wait_recv()
    joined = lambda ref: jnp.concatenate([ref[0], ref[1]], axis=-1)
    w_qg = jnp.concatenate([joined(wq_v), joined(wg_v)], axis=1)
    w_kv = jnp.concatenate([joined(wk_v), joined(wv_v)], axis=1)
    queried = normed_v[:, pl.ds(pl.multiple_of(core * part, part), part), :]
    queried = queried.reshape(local_rows * part, channels)
    projected_qg = jnp.dot(queried, w_qg, preferred_element_type=f32)
    projected_kv = jnp.dot(normed, w_kv, preferred_element_type=f32)
    query = (projected_qg[:, :LANES] * HD ** (-0.5)).astype(bf16)
    gate = jax.nn.sigmoid(projected_qg[:, LANES:] + joined(gb_v))
    keys_all = projected_kv[:, :LANES].astype(bf16)
    values_all = projected_kv[:, LANES:].astype(bf16)
    out_full = wo_v[...].reshape(2 * inner, channels)
    heads = LANES // HD
    same = (
        lax.broadcasted_iota(jnp.int32, (LANES, LANES), 0) // width
        == lax.broadcasted_iota(jnp.int32, (LANES, LANES), 1) // HD
    )
    ones = jnp.where(same, 1.0, 0.0).astype(bf16)
    mask_f = (mask_v[...].astype(f32) - 1.0) * MASK_WEIGHT
    mask_add = jnp.concatenate([mask_f] * heads, axis=1)
    scores, mixers = [], []
    for i in range(local_rows):
        rows = slice(i * width, (i + 1) * width)
        spread_keys = jnp.concatenate([keys_all[rows]] * heads, axis=0) * ones
        spread_values = jnp.concatenate([values_all[rows]] * heads, axis=0) * ones
        mixers.append(jnp.concatenate([spread_values, ones], axis=1))
        scores.append(
            lax.dot_general(
                query[i * part : (i + 1) * part],
                spread_keys,
                (((1,), (1,)), ((), ())),
                preferred_element_type=f32,
            )
            + mask_add
        )

    for slot in range(n_row):
        src_row, src_core = core * per_half + slot // 2, slot % 2

        @pl.when(jnp.logical_or(src_row != row, src_core != core))
        def _():
            pltpu.make_async_remote_copy(
                src_ref=message,
                dst_ref=received.at[slot],
                send_sem=b_send.at[slot],
                recv_sem=b_recv.at[slot],
                device_id={"row": row, "head": other},
                device_id_type=MESH,
            ).wait_recv()

    tiles = []
    for t in range(part // SUBLANES):
        first = t * per_tile * 2
        total = received[first]
        for s in range(1, per_tile * 2):
            total = total + received[first + s]
        tiles.append(total)
    bias = jnp.concatenate(tiles, axis=0)
    segment = lax.broadcasted_iota(jnp.int32, (part, LANES), 1) // width
    attended = []
    for i in range(local_rows):
        full = scores[i] + bias
        highest = None
        for h in range(heads):
            inside = segment == h
            top = jnp.max(jnp.where(inside, full, -jnp.inf), axis=-1, keepdims=True)
            highest = top if highest is None else jnp.where(inside, top, highest)
        exponent = jnp.exp(full - highest).astype(bf16)
        mixed = jnp.dot(exponent, mixers[i], preferred_element_type=f32)
        attended.append(mixed[:, :LANES] / mixed[:, LANES:])
    attended = jnp.concatenate(attended, axis=0)
    gated = (gate * attended).astype(bf16)
    result = jnp.dot(gated, out_full, preferred_element_type=f32) + ob_v[...]
    out_ref[...] = result.astype(bf16).reshape(out_ref.shape)

    for copy in weights:
        copy.wait_send()
    for turn in range(1, n_row):
        bias_copy(turn).wait_send()

    @pl.when(half != core)
    def _():
        bias_copy(0).wait_send()


def packed_local(
    n_row, pair, mask, ln_gain, ln_bias, w_query, w_key, w_value, w_bias, w_gate, gate_bias, w_out, out_bias
):
    local_rows, width, channels = pair.shape
    bf16, f32 = jnp.bfloat16, jnp.float32
    vmem = pltpu.VMEM
    args = (
        pair,
        mask[None],
        ln_gain[None],
        ln_bias[None],
        w_query,
        w_key,
        w_value,
        w_bias,
        w_gate,
        gate_bias[None],
        w_out,
        out_bias[None],
    )
    pairs = lambda a: vmem((2,) + a.shape, a.dtype)
    single = lambda a: vmem(a.shape, a.dtype)
    shared = {4, 5, 6, 8, 9, 10}
    return pl.pallas_call(
        functools.partial(packed_kernel, n_row),
        out_shape=jax.ShapeDtypeStruct((local_rows, width // 2, channels), bf16),
        in_specs=[pl.BlockSpec(memory_space=pltpu.HBM)] * len(args),
        out_specs=pl.BlockSpec(memory_space=vmem),
        scratch_shapes=[pairs(a) if i in shared else single(a) for i, a in enumerate(args)]
        + [
            vmem((local_rows, width, channels), bf16),
            vmem((SUBLANES, LANES), f32),
            vmem((n_row, SUBLANES, LANES), f32),
            pltpu.SemaphoreType.DMA((len(args),)),
            pltpu.SemaphoreType.DMA((6,)),
            pltpu.SemaphoreType.DMA((6,)),
            pltpu.SemaphoreType.DMA((n_row,)),
            pltpu.SemaphoreType.DMA((n_row,)),
        ],
        compiler_params=pltpu.CompilerParams(collective_id=0, has_side_effects=True),
    )(*args)


def solution(mesh):
    placed = (
        P(("groups", "row"), None, None),
        P("groups"),
        P(),
        P(),
        P(None, "head"),
        P(None, "head"),
        P(None, "head"),
        P(None, "head"),
        P(None, "head"),
        P("head"),
        P("head", None),
        P(),
    )
    out_placed = P(("groups", "row"), "head", None)

    def call(pair, mask, ln_gain, ln_bias, w_query, *rest):
        packed = packs(mesh, pair, w_query)
        body = functools.partial(packed_local, mesh.shape["row"]) if packed else local
        return jax.shard_map(
            body, mesh=mesh, in_specs=placed, out_specs=out_placed, check_vma=False
        )(pair, mask, ln_gain, ln_bias, w_query, *rest)

    return call
```

```python
import functools
import math

import jax
import jax.numpy as jnp
from jax import lax
from jax.experimental import pallas as pl
from jax.experimental.pallas import tpu as pltpu
from jax.sharding import PartitionSpec as P

HD = 32


EPSILON = 1e-05
MASK_WEIGHT = 1000000000.0


def layer_normed(pair_rows, ln_gain, ln_bias):
    values_f = pair_rows.astype(jnp.float32)
    average = jnp.mean(values_f, axis=-1, keepdims=True)
    centred = values_f - average
    variance = jnp.mean(centred * centred, axis=-1, keepdims=True)
    scaled = centred * lax.rsqrt(variance + EPSILON) * ln_gain + ln_bias
    return scaled.astype(jnp.bfloat16)


def attend_rows(result, bias_block, offset, query, keys_all, values_all, mask_add):
    sub_rows = bias_block.shape[1]
    query_block = lax.dynamic_slice_in_dim(query, offset, sub_rows, 1)
    scores = jnp.einsum(
        "ijhd,ikhd->ihjk", query_block, keys_all, preferred_element_type=jnp.float32
    )
    scores = scores + bias_block[None] + mask_add
    highest = jnp.max(scores, axis=-1, keepdims=True)
    exponent = jnp.exp(scores - highest)
    weights = (exponent / jnp.sum(exponent, axis=-1, keepdims=True)).astype(jnp.bfloat16)
    attended = jnp.einsum(
        "ihjk,ikhd->ijhd", weights, values_all, preferred_element_type=jnp.float32
    )
    return lax.dynamic_update_slice_in_dim(result, attended, offset, 1)


def attend_block(carry, piece, start, block_rows, query, keys_all, values_all, mask_add):
    count = piece.shape[1]

    def one_step(turn, result):
        offset = turn * block_rows
        bias_block = lax.dynamic_slice_in_dim(piece, offset, block_rows, 1)
        return attend_rows(
            result, bias_block, start + offset, query, keys_all, values_all, mask_add
        )

    return lax.fori_loop(0, count // block_rows, one_step, carry)


def local(
    pair,
    mask,
    ln_gain,
    ln_bias,
    w_query,
    w_key,
    w_value,
    w_bias,
    w_gate,
    gate_bias,
    w_out,
    out_bias,
):
    local_rows, width_all, channels = pair.shape
    normed = layer_normed(pair, ln_gain, ln_bias)
    flat = normed.reshape(-1, channels)
    inner_width = w_query.shape[1]
    heads_local = inner_width // HD
    joined = jnp.concatenate([w_query, w_key, w_value, w_gate], axis=1)
    projected = jnp.dot(flat, joined, preferred_element_type=jnp.float32)
    four_shape = (local_rows, width_all, heads_local, HD)
    query = (projected[:, :inner_width] * HD ** (-0.5)).astype(jnp.bfloat16).reshape(four_shape)
    keys_all = projected[:, inner_width : 2 * inner_width].astype(jnp.bfloat16).reshape(four_shape)
    values_all = (
        projected[:, 2 * inner_width : 3 * inner_width].astype(jnp.bfloat16).reshape(four_shape)
    )
    gate = jax.nn.sigmoid(projected[:, 3 * inner_width :] + gate_bias)
    bias_local = jnp.dot(flat, w_bias, preferred_element_type=jnp.float32)
    bias_local = jnp.transpose(bias_local.reshape(local_rows, width_all, heads_local), (2, 0, 1))
    mask_add = (mask.astype(jnp.float32) - 1.0) * MASK_WEIGHT
    block_rows = math.gcd(width_all, 64)
    empty = jnp.zeros(four_shape, jnp.float32)
    bias_every = lax.all_gather(bias_local, "row", axis=1, tiled=True)
    attended = attend_block(empty, bias_every, 0, block_rows, query, keys_all, values_all, mask_add)
    gated = (gate * attended.reshape(-1, inner_width)).astype(jnp.bfloat16)
    traded = lax.all_to_all(
        gated.reshape(local_rows, width_all, inner_width),
        "head",
        split_axis=1,
        concat_axis=2,
        tiled=True,
    )
    out_full = lax.all_gather(w_out, "head", axis=0, tiled=True)
    mixed = jnp.dot(
        traded.reshape(-1, traded.shape[2]), out_full, preferred_element_type=jnp.float32
    )
    mixed = mixed.reshape(local_rows, traded.shape[1], channels)
    return (mixed + out_bias).astype(jnp.bfloat16)


LANES = 128
SUBLANES = 8
MESH = pl.DeviceIdType.MESH


def packs(mesh, pair, w_query):
    rows, heads = mesh.shape["row"], mesh.shape["head"]
    part_rows = pair.shape[0] // mesh.shape["groups"]
    width, channels = pair.shape[1:]
    local_rows = part_rows // rows
    return (
        heads == 2
        and part_rows == width
        and rows % heads == 0
        and SUBLANES % local_rows == 0
        and width % (16 * heads) == 0
        and channels == LANES
        and w_query.shape[1] == LANES
        and (LANES // HD) * width == LANES
    )


def dot_lanes(left, right):
    return lax.dot_general(
        left, right, (((1,), (1,)), ((), ())), preferred_element_type=jnp.float32
    )


def packed_kernel(
    n_row,
    pair_h,
    mask_h,
    gain_h,
    shift_h,
    wq_h,
    wk_h,
    wv_h,
    wb_h,
    wg_h,
    gb_h,
    wo_h,
    ob_h,
    out_ref,
    pair_v,
    mask_v,
    gain_v,
    shift_v,
    wq_v,
    wk_v,
    wv_v,
    wb_v,
    wg_v,
    gb_v,
    wo_v,
    ob_v,
    normed_v,
    message,
    received,
    in_sem,
    w_send,
    w_recv,
    b_send,
    b_recv,
):
    row, core = lax.axis_index("row"), lax.axis_index("head")
    other = 1 - core
    local_rows, width, channels = pair_v.shape
    inner = wq_v.shape[1]
    part = width // 2
    per_half = n_row // 2
    half = row // per_half
    heads_local = wb_v.shape[0]
    f32, bf16 = jnp.float32, jnp.bfloat16

    barrier = pltpu.get_barrier_semaphore()
    for slot in range(n_row):
        src_row, src_core = core * per_half + slot // 2, slot % 2

        @pl.when(jnp.logical_or(src_row != row, src_core != core))
        def _():
            pl.semaphore_signal(
                barrier,
                inc=1,
                device_id={"row": src_row, "head": src_core},
                device_id_type=MESH,
            )

    @pl.when(half != core)
    def _():
        pl.semaphore_signal(
            barrier, inc=1, device_id={"row": row, "head": other}, device_id_type=MESH
        )

    locals_ = [
        pltpu.make_async_copy(src, dst, in_sem.at[i])
        for i, (src, dst) in enumerate(
            (
                (pair_h, pair_v),
                (gain_h, gain_v),
                (shift_h, shift_v),
                (wb_h, wb_v),
                (mask_h, mask_v),
                (ob_h, ob_v),
                (wk_h, wk_v.at[core]),
                (wq_h, wq_v.at[core]),
                (wv_h, wv_v.at[core]),
                (wg_h, wg_v.at[core]),
                (gb_h, gb_v.at[core]),
                (wo_h, wo_v.at[core]),
            )
        )
    ]
    for copy in locals_:
        copy.start()
    weights = [
        pltpu.make_async_remote_copy(
            src_ref=src,
            dst_ref=dst.at[core],
            send_sem=w_send.at[i],
            recv_sem=w_recv.at[i],
            device_id={"row": row, "head": other},
            device_id_type=MESH,
        )
        for i, (src, dst) in enumerate(
            (
                (wk_h, wk_v),
                (wq_h, wq_v),
                (wv_h, wv_v),
                (wg_h, wg_v),
                (gb_h, gb_v),
                (wo_h, wo_v),
            )
        )
    ]

    for copy in locals_[:4]:
        copy.wait()
    row_head = lax.broadcasted_iota(jnp.int32, (LANES, channels), 0) // width
    wb = wb_v[...]
    spread = jnp.zeros((LANES, channels), f32)
    for h in range(heads_local):
        spread = jnp.where(
            row_head == core * heads_local + h, wb[h : h + 1].astype(f32), spread
        )
    spread = spread.astype(bf16)
    values_f = pair_v[...].astype(f32).reshape(local_rows * width, channels)
    average = jnp.mean(values_f, axis=-1, keepdims=True)
    centred = values_f - average
    variance = jnp.mean(centred * centred, axis=-1, keepdims=True)
    normed = (centred * lax.rsqrt(variance + EPSILON) * gain_v[...] + shift_v[...]).astype(bf16)
    normed_v[...] = normed.reshape(local_rows, width, channels)

    product = dot_lanes(normed, spread)
    tokens = local_rows * width
    token_key = lax.broadcasted_iota(jnp.int32, (tokens, LANES), 0) % width
    lane_key = lax.broadcasted_iota(jnp.int32, (tokens, LANES), 1) % width
    product = jnp.where(token_key == lane_key, product, 0.0)
    reduced = jnp.sum(product.reshape(local_rows, width, LANES), axis=1)
    per_tile = SUBLANES // local_rows
    sublane = lax.broadcasted_iota(jnp.int32, (SUBLANES, LANES), 0)
    tile = jnp.zeros((SUBLANES, LANES), f32)
    for j in range(local_rows):
        tile = jnp.where(sublane == (row % per_tile) * local_rows + j, reduced[j : j + 1], tile)
    message[...] = tile

    pl.semaphore_wait(barrier, n_row)
    slot_mine = (row % per_half) * 2 + core

    def bias_copy(turn):
        return pltpu.make_async_remote_copy(
            src_ref=message,
            dst_ref=received.at[slot_mine],
            send_sem=b_send.at[turn],
            recv_sem=b_recv.at[slot_mine],
            device_id={"row": lax.rem(row + turn, n_row), "head": half},
            device_id_type=MESH,
        )

    for turn in reversed(range(1, n_row)):
        bias_copy(turn).start()

    @pl.when(half != core)
    def _():
        bias_copy(0).start()

    for copy in weights:
        copy.start()

    @pl.when(half == core)
    def _():
        received[slot_mine] = tile

    for copy in locals_[4:]:
        copy.wait()
    for copy in weights:
        copy.wait_recv()
    stacked = lambda ref: ref[...].reshape(2 * inner, channels)
    w_qg = jnp.concatenate([stacked(wq_v), stacked(wg_v)], axis=0)
    w_kv = jnp.concatenate([stacked(wk_v), stacked(wv_v)], axis=0)
    queried = normed_v[:, pl.ds(pl.multiple_of(core * part, part), part), :]
    queried = queried.reshape(local_rows * part, channels)
    projected_qg = dot_lanes(queried, w_qg)
    projected_kv = dot_lanes(normed, w_kv)
    query = (projected_qg[:, :LANES] * HD ** (-0.5)).astype(bf16)
    gate = jax.nn.sigmoid(projected_qg[:, LANES:] + jnp.concatenate([gb_v[0], gb_v[1]], axis=-1))
    keys_all = projected_kv[:, :LANES].astype(bf16)
    values_all = projected_kv[:, LANES:].astype(bf16)
    out_full = stacked(wo_v)
    heads = LANES // HD
    same = (
        lax.broadcasted_iota(jnp.int32, (LANES, LANES), 0) // width
        == lax.broadcasted_iota(jnp.int32, (LANES, LANES), 1) // HD
    )
    ones = jnp.where(same, 1.0, 0.0).astype(bf16)
    mask_f = (mask_v[...].astype(f32) - 1.0) * MASK_WEIGHT
    mask_add = jnp.concatenate([mask_f] * heads, axis=1)
    scores, mixers = [], []
    for i in range(local_rows):
        rows = slice(i * width, (i + 1) * width)
        spread_keys = jnp.concatenate([keys_all[rows]] * heads, axis=0) * ones
        spread_values = jnp.concatenate([values_all[rows]] * heads, axis=0) * ones
        mixers.append(jnp.concatenate([spread_values, ones], axis=1))
        scores.append(
            dot_lanes(query[i * part : (i + 1) * part], spread_keys) + mask_add
        )

    for slot in range(n_row):
        src_row, src_core = core * per_half + slot // 2, slot % 2

        @pl.when(jnp.logical_or(src_row != row, src_core != core))
        def _():
            pltpu.make_async_remote_copy(
                src_ref=message,
                dst_ref=received.at[slot],
                send_sem=b_send.at[slot],
                recv_sem=b_recv.at[slot],
                device_id={"row": row, "head": other},
                device_id_type=MESH,
            ).wait_recv()

    tiles = []
    for t in range(part // SUBLANES):
        first = t * per_tile * 2
        total = received[first]
        for s in range(1, per_tile * 2):
            total = total + received[first + s]
        tiles.append(total)
    bias = jnp.concatenate(tiles, axis=0)
    segment = lax.broadcasted_iota(jnp.int32, (part, LANES), 1) // width
    attended = []
    for i in range(local_rows):
        full = scores[i] + bias
        highest = None
        for h in range(heads):
            inside = segment == h
            top = jnp.max(jnp.where(inside, full, -jnp.inf), axis=-1, keepdims=True)
            highest = top if highest is None else jnp.where(inside, top, highest)
        exponent = jnp.exp(full - highest).astype(bf16)
        mixed = jnp.dot(exponent, mixers[i], preferred_element_type=f32)
        attended.append(mixed[:, :LANES] / mixed[:, LANES:])
    attended = jnp.concatenate(attended, axis=0)
    gated = (gate * attended).astype(bf16)
    result = jnp.dot(gated, out_full, preferred_element_type=f32) + ob_v[...]
    out_ref[...] = result.astype(bf16).reshape(out_ref.shape)

    for copy in weights:
        copy.wait_send()
    for turn in range(1, n_row):
        bias_copy(turn).wait_send()

    @pl.when(half != core)
    def _():
        bias_copy(0).wait_send()


def packed_local(
    n_row, pair, mask, ln_gain, ln_bias, w_query, w_key, w_value, w_bias, w_gate, gate_bias, w_out, out_bias
):
    local_rows, width, channels = pair.shape
    bf16, f32 = jnp.bfloat16, jnp.float32
    vmem = pltpu.VMEM
    args = (
        pair,
        mask[None],
        ln_gain[None],
        ln_bias[None],
        w_query.T,
        w_key.T,
        w_value.T,
        w_bias.T,
        w_gate.T,
        gate_bias[None],
        w_out,
        out_bias[None],
    )
    pairs = lambda a: vmem((2,) + a.shape, a.dtype)
    single = lambda a: vmem(a.shape, a.dtype)
    shared = {4, 5, 6, 8, 9, 10}
    return pl.pallas_call(
        functools.partial(packed_kernel, n_row),
        out_shape=vmem((local_rows, width // 2, channels), bf16),
        in_specs=[pl.BlockSpec(memory_space=pltpu.HBM)] * len(args),
        out_specs=pl.BlockSpec(memory_space=vmem),
        scratch_shapes=[pairs(a) if i in shared else single(a) for i, a in enumerate(args)]
        + [
            vmem((local_rows, width, channels), bf16),
            vmem((SUBLANES, LANES), f32),
            vmem((n_row, SUBLANES, LANES), f32),
            pltpu.SemaphoreType.DMA((len(args),)),
            pltpu.SemaphoreType.DMA((6,)),
            pltpu.SemaphoreType.DMA((6,)),
            pltpu.SemaphoreType.DMA((n_row,)),
            pltpu.SemaphoreType.DMA((n_row,)),
        ],
        compiler_params=pltpu.CompilerParams(collective_id=0, has_side_effects=True),
    )(*args)


def solution(mesh):
    placed = (
        P(("groups", "row"), None, None),
        P("groups"),
        P(),
        P(),
        P(None, "head"),
        P(None, "head"),
        P(None, "head"),
        P(None, "head"),
        P(None, "head"),
        P("head"),
        P("head", None),
        P(),
    )
    out_placed = P(("groups", "row"), "head", None)

    def call(pair, mask, ln_gain, ln_bias, w_query, *rest):
        packed = packs(mesh, pair, w_query)
        body = functools.partial(packed_local, mesh.shape["row"]) if packed else local
        return jax.shard_map(
            body, mesh=mesh, in_specs=placed, out_specs=out_placed, check_vma=False
        )(pair, mask, ln_gain, ln_bias, w_query, *rest)

    return call
```
